1024 devices in a mesh: group: 4 (over y_hi), dp: 16 (over y_lo, z), tensor: 16 (over x, core).
Axes of the slice: x: 8, y: 8 (y_hi: 4, y_lo: 2; y = y_hi * 2 + y_lo), z: 8, core: 2. Of those that a mesh axis runs over, the one named last changes fastest.
Arguments:
- queries: bfloat16 [256, 4, 8192], P(('group', 'dp')), may hold values from -330 to 330
- keys: bfloat16 [256, 8, 2048, 128], P(('group', 'dp'), None, 'tensor'), may hold values from -12 to 12
- values: bfloat16 [256, 8, 2048, 128], P(('group', 'dp'), None, 'tensor'), may hold values from -12 to 12
- cached_length: int32 [256], P(('group', 'dp')), may hold values from 2 to 2044
- out_weight: bfloat16 [8192, 8192], P('tensor', ('group', 'dp')), may hold values from -0.0625 to 0.0625
Outputs:
- projected: bfloat16 [1024, 4, 2048], P(('group', 'tensor'), None, 'dp')
The draws below stay inside these ranges and needn't reach their ends.
Inputs may be any that keep to these rules, and one draw needn't show every extreme that they name: The keys and values of row r's 4 new tokens sit at positions cached_length[r] to cached_length[r] + 3.
All inputs are finite; a program needn't handle non-finite values.
Results may differ from the reference program's by a relative error of at most 0.018.
Values may be sent and summed in bfloat16 or wider, within the bound.
A program may use at most 32 MiB of HBM per device.

```python
import math
import jax
import jax.numpy as jnp
from jax import lax

MODEL_DIM = 8192
QUERY_HEADS = 64
KEY_VALUE_HEADS = 8
HEAD_SIZE = 128
ROWS_PER_SHARD = 4
NEW_TOKENS = 4
BATCH_ROWS = 256
CACHE_CAPACITY = 2048
TOKENS = 1024
N_GROUP = 4


def joint_draw(key):
    query_key, cache_draw_key = jax.random.split(jax.random.fold_in(key, 17))
    key_cache_rows = jnp.clip(jax.random.normal(cache_draw_key, (BATCH_ROWS, KEY_VALUE_HEADS, CACHE_CAPACITY, HEAD_SIZE), jnp.float32), -4.0, 4.0)
    query_all = jnp.clip(2.5 * jax.random.normal(query_key, (BATCH_ROWS, NEW_TOKENS, QUERY_HEADS, HEAD_SIZE), jnp.float32), -10.0, 10.0)
    return (query_all.reshape(BATCH_ROWS, NEW_TOKENS, QUERY_HEADS * HEAD_SIZE), key_cache_rows)


def draw_queries(key, part):
    return joint_draw(key)[0].astype(jnp.bfloat16)


def draw_keys(key, part):
    return joint_draw(key)[1].astype(jnp.bfloat16)


def touch_ends(values, key, least, largest):
    place = [jax.random.randint(jax.random.fold_in(key, axis), (), 0, length) for axis, length in enumerate(values.shape)]
    longest = values.shape.index(max(values.shape))
    neighbour = place[:longest] + [(place[longest] + 1) % values.shape[longest]] + place[longest + 1:]
    return values.at[tuple(place)].set(least).at[tuple(neighbour)].set(largest)


def block_levels(stream_key, extent, shards, least, largest):
    loudness = 1.0
    for axis_at, parts in shards:
        steps = jax.random.uniform(jax.random.fold_in(jax.random.fold_in(stream_key, 6), axis_at), (parts,), jnp.float32, least / len(shards), largest / len(shards))
        loudness = loudness * jnp.repeat(jnp.exp(steps), extent[axis_at] // parts).reshape((-1,) + (1,) * (len(extent) - 1 - axis_at))
    return loudness


def normal_values(rng, shape, scale, most, cuts=(), kind=jnp.bfloat16):
    entries = jax.random.normal(rng, shape, jnp.float32) * scale
    if len(cuts) > 0:
        entries = block_levels(rng, shape, cuts, -0.22, 0.18) * entries
    return jnp.clip(entries, min=-most, max=most).astype(kind)


def setup_inputs(seed: int = 0) -> dict:
    key_of = jax.random.split(jax.random.key(seed), 6)
    return {
        "queries": draw_queries(jax.random.fold_in(key_of[5], 71), 0),
        "keys": draw_keys(jax.random.fold_in(key_of[5], 71), 0),
        "values": normal_values(key_of[2], (BATCH_ROWS, KEY_VALUE_HEADS, CACHE_CAPACITY, HEAD_SIZE), 2.0, 12.0, ((0, 64), (2, 16))),
        "cached_length": touch_ends(jax.random.randint(key_of[3], (BATCH_ROWS,), 2, CACHE_CAPACITY - NEW_TOKENS + 1), jax.random.fold_in(key_of[3], 1), 2, CACHE_CAPACITY - NEW_TOKENS).astype(jnp.int32),
        "out_weight": normal_values(key_of[4], (MODEL_DIM, MODEL_DIM), MODEL_DIM ** -0.5, 0.0625, ((0, 16), (1, 64))),
    }


def attend_row_block(inputs):
    query_matrix, key_rows, value_rows, length_rows = inputs
    batch_row_count = query_matrix.shape[0]
    heads_per_group = QUERY_HEADS // KEY_VALUE_HEADS
    reshaped_output = query_matrix.astype(jnp.float32).reshape(batch_row_count, NEW_TOKENS, KEY_VALUE_HEADS, heads_per_group, HEAD_SIZE)
    scores = jnp.einsum('rsgjd,rgpd->rgsjp', reshaped_output, key_rows.astype(jnp.float32)) / math.sqrt(HEAD_SIZE)
    position = jnp.arange(CACHE_CAPACITY, dtype=jnp.int32)
    horizon = length_rows[:, None] + jnp.arange(NEW_TOKENS, dtype=jnp.int32)[None, :] + 1
    allowed = position[None, None, None, None, :] < horizon[:, None, :, None, None]
    masked = jnp.where(allowed, scores, -1e+30)
    row_top = lax.optimization_barrier(jnp.max(masked, axis=-1, keepdims=True))
    exponent = jnp.where(allowed, jnp.exp(masked - row_top), 0.0)
    totals = lax.optimization_barrier(jnp.sum(exponent, axis=-1))
    rounded = lax.optimization_barrier(exponent.astype(jnp.bfloat16)).astype(jnp.float32)
    weighted = jnp.einsum('rgsjp,rgpd->rsgjd', rounded, value_rows.astype(jnp.float32))
    attended_output = weighted / jnp.transpose(totals, (0, 2, 1, 3))[..., None]
    return attended_output.reshape(batch_row_count, NEW_TOKENS, MODEL_DIM).astype(jnp.bfloat16)

def reference(queries, keys, values, cached_length, out_weight):
    row_blocks = BATCH_ROWS // ROWS_PER_SHARD
    attended_output = lax.map(attend_row_block, (queries.reshape(row_blocks, ROWS_PER_SHARD, NEW_TOKENS, MODEL_DIM), keys.reshape(row_blocks, ROWS_PER_SHARD, KEY_VALUE_HEADS, CACHE_CAPACITY, HEAD_SIZE), values.reshape(row_blocks, ROWS_PER_SHARD, KEY_VALUE_HEADS, CACHE_CAPACITY, HEAD_SIZE), cached_length.reshape(row_blocks, ROWS_PER_SHARD)))
    attended_output = attended_output.reshape(TOKENS, MODEL_DIM)
    projected = jnp.dot(attended_output, out_weight, preferred_element_type=jnp.float32).astype(jnp.bfloat16)
    return projected.reshape(TOKENS, N_GROUP, MODEL_DIM // N_GROUP)
```

```python
import functools
import math

import jax
import jax.numpy as jnp
from jax import lax
from jax.experimental import pallas as pl
from jax.experimental.pallas import tpu as pltpu
from jax.sharding import PartitionSpec as P

MESH = pl.DeviceIdType.MESH
F32 = jnp.float32
BF16 = jnp.bfloat16
FAR_FIRST = (4, 3, 5, 2, 6, 1, 7)
NEAR_FIRST = (1, 7, 2, 6, 3, 5, 4)


def remote(src, dst, send, recv, device):
    return pltpu.make_async_remote_copy(
        src_ref=src, dst_ref=dst, send_sem=send, recv_sem=recv, device_id=device, device_id_type=MESH
    )


def kernel(
    length_ref,
    q_hbm,
    k_hbm,
    v_hbm,
    w_hbm,
    out_ref,
    q_v,
    k_v,
    v_v,
    w_v,
    pair_o,
    pair_st,
    got_o,
    got_st,
    own_w,
    own_st,
    a_o,
    a_st,
    ar_o,
    ar_st,
    x_all,
    e_o,
    er_o,
    load_sem,
    wload_sem,
    pair_send,
    pair_recv,
    w_send,
    w_recv,
    a_send,
    a_recv,
    ast_send,
    ast_recv,
    d_send,
    d_recv,
    y_send,
    y_recv,
    e_send,
    e_recv,
):
    g = lax.axis_index("group")
    d = lax.axis_index("dp")
    t = lax.axis_index("tensor")
    x, c = t // 2, t % 2
    other = 1 - c
    ylo, z = d // 8, d % 8
    mate = {"tensor": x * 2 + other}
    y_mate = {"dp": (1 - ylo) * 8 + z}
    right = {"group": (g + 1) % 4}
    left = {"group": (g + 3) % 4}

    def along_x(step, core):
        return {"tensor": ((x + step) % 8) * 2 + core}

    def along_z(step):
        return {"dp": ylo * 8 + (z + step) % 8}

    loads = []
    for slot, half in ((0, other), (1, c)):
        rows = pl.ds(half * 2, 2)
        for which, (src, dst) in enumerate(((q_hbm, q_v), (k_hbm, k_v), (v_hbm, v_v))):
            copy = pltpu.make_async_copy(src.at[rows], dst.at[slot], load_sem.at[slot, which])
            copy.start()
            loads.append(copy)
    w_load = pltpu.make_async_copy(w_hbm, w_v.at[c, g], wload_sem)
    w_load.start()

    barrier = pltpu.get_barrier_semaphore()
    peers = [mate, y_mate, right, left]
    for step in range(1, 8):
        peers += [along_x(step, 0), along_x(step, 1), along_z(step)]
    for peer in peers:
        pl.semaphore_signal(barrier, inc=1, device_id=peer, device_id_type=MESH)

    lane = lax.broadcasted_iota(jnp.int32, (64, 128), 1)
    row = lax.broadcasted_iota(jnp.int32, (64, 128), 0)
    first_row = (row // 4) % 2 == 0
    low_eye = lane == row
    high_eye = lane == row + 64
    position = t * 128 + lane
    scale = 1.0 / math.sqrt(128)

    def attend(slot, half, k, allowed):
        pair = jnp.concatenate(
            [q_v[slot, r, :, k * 1024 : (k + 1) * 1024].astype(F32) for r in range(2)], axis=0
        )
        q = jnp.concatenate([pair[:, j * 128 : (j + 1) * 128] for j in range(8)], axis=0).astype(BF16)
        keys = jnp.concatenate([k_v[slot, 0, k], k_v[slot, 1, k]], axis=0)
        vals = jnp.concatenate([v_v[slot, 0, k], v_v[slot, 1, k]], axis=0)
        s = lax.dot_general(q, keys, (((1,), (1,)), ((), ())), preferred_element_type=F32)
        s = jnp.where(first_row, s[:, :128], s[:, 128:]) * scale
        s = jnp.where(allowed, s, -1e30)
        m = jnp.max(s, axis=1, keepdims=True)
        p = jnp.where(allowed, jnp.exp(s - m), 0.0)
        l = jnp.sum(p, axis=1, keepdims=True)
        both = jnp.concatenate(
            [jnp.where(first_row, p, 0.0), jnp.where(first_row, 0.0, p)], axis=1
        ).astype(BF16)
        w = jnp.dot(both, vals, preferred_element_type=F32)
        stats = jnp.where(low_eye, m, jnp.where(high_eye, l, 0.0))
        return w, jnp.sum(stats, axis=0, keepdims=True)

    def mask_of(half):
        horizon = jnp.where(first_row, length_ref[half * 2], length_ref[half * 2 + 1]) + row % 4 + 1
        return position < horizon

    for copy in loads[:3]:
        copy.wait()
    allowed = mask_of(other)
    for k in range(8):
        w, stats = attend(0, other, k, allowed)
        pair_o[k] = w.astype(BF16)
        pair_st[k : k + 1] = stats

    w_load.wait()
    pl.semaphore_wait(barrier, len(peers))

    pair_copies = [
        remote(pair_o, got_o, pair_send.at[0], pair_recv.at[0], mate),
        remote(pair_st, got_st, pair_send.at[1], pair_recv.at[1], mate),
    ]
    for copy in pair_copies:
        copy.start()

    top, bottom = pl.ds(0, 256), pl.ds(256, 256)

    def w_copy(block, part, index, device):
        ref = w_v.at[c, block, part]
        return remote(ref, ref, w_send.at[index], w_recv.at[index], device)

    w_top_right = w_copy(g, top, 0, right)
    w_bottom_left = w_copy(g, bottom, 1, left)
    w_bottom_right = w_copy(g, bottom, 2, right)
    w_top_left = w_copy(g, top, 3, left)
    for copy in (w_top_right, w_bottom_left, w_bottom_right, w_top_left):
        copy.start()

    for copy in loads[3:]:
        copy.wait()
    allowed = mask_of(c)
    for k in range(8):
        w, stats = attend(1, c, k, allowed)
        own_w[k] = w
        own_st[k : k + 1] = stats

    def w_to_mate(block, index):
        ref = w_v.at[c, block]
        return remote(ref, ref, w_send.at[index], w_recv.at[index], mate)

    w_mates = [w_to_mate(g, 6)]
    w_mates[0].start()

    for copy in pair_copies:
        copy.wait_recv()
    st1, st2 = own_st[...], got_st[...]
    low = lax.broadcasted_iota(jnp.int32, (8, 128), 1) < 64
    top_both = jnp.maximum(st1, st2)
    e1, e2 = jnp.exp(st1 - top_both), jnp.exp(st2 - top_both)
    total = e1 * pltpu.roll(st1, 64, 1) + e2 * pltpu.roll(st2, 64, 1)
    merged = jnp.where(low, top_both, pltpu.roll(total, 64, 1))
    factors = jnp.where(low, e1, pltpu.roll(e2, 64, 1))
    for k in range(8):
        f = factors[k : k + 1]
        f1 = jnp.sum(jnp.where(low_eye, f, 0.0), axis=1, keepdims=True)
        f2 = jnp.sum(jnp.where(high_eye, f, 0.0), axis=1, keepdims=True)
        a_o[k] = (f1 * own_w[k] + f2 * got_o[k].astype(F32)).astype(BF16)
        a_st[k] = merged[k : k + 1]

    a_copies = []
    for step in FAR_FIRST:
        head = (x + step) % 8
        a_copies.append(remote(a_o.at[head], ar_o.at[step], a_send.at[step], a_recv.at[step], along_x(step, c)))
        a_copies.append(
            remote(a_st.at[head], ar_st.at[step], ast_send.at[step], ast_recv.at[step], along_x(step, c))
        )
    for copy in a_copies:
        copy.start()

    w_top_right.wait_recv()
    w_on_right = w_copy((g + 3) % 4, top, 4, right)
    w_on_right.start()
    w_bottom_left.wait_recv()
    w_on_left = w_copy((g + 1) % 4, bottom, 5, left)
    w_on_left.start()

    for copy in a_copies:
        copy.wait_recv()
    st = jnp.concatenate([a_st[x]] + [ar_st[i] for i in range(1, 8)], axis=0)
    m = jnp.max(st, axis=0, keepdims=True)
    e = jnp.exp(st - m)
    total = jnp.sum(e * pltpu.roll(st, 64, 1), axis=0, keepdims=True)
    f = e / total
    attended = jnp.zeros((64, 128), F32)
    for i in range(8):
        part = a_o[x] if i == 0 else ar_o[i]
        fi = jnp.sum(jnp.where(low_eye, f[i : i + 1], 0.0), axis=1, keepdims=True)
        attended += fi * part.astype(F32)
    for j in range(8):
        x_all[d, :, j * 128 : (j + 1) * 128] = attended[j * 8 : (j + 1) * 8].astype(BF16)

    def d_copy(slot, send, recv, device):
        ref = x_all.at[slot]
        return remote(ref, ref, send, recv, device)

    d_copies = {step: d_copy(d, d_send.at[step], d_recv.at[step], along_z(step)) for step in range(1, 8)}
    y_copies = [d_copy(d, y_send.at[0], y_recv.at[0], y_mate)]
    for step in FAR_FIRST:
        d_copies[step].start()
    y_copies[0].start()

    w_bottom_right.wait_recv()
    w_mates.append(w_to_mate((g + 3) % 4, 7))
    w_mates[1].start()
    w_top_left.wait_recv()
    w_mates.append(w_to_mate((g + 1) % 4, 8))
    w_mates[2].start()

    for step in NEAR_FIRST:
        d_copies[step].wait_recv()
        came = ylo * 8 + (z + 8 - step) % 8
        y_copies.append(d_copy(came, y_send.at[step], y_recv.at[step], y_mate))
        y_copies[-1].start()

    w_on_right.wait_recv()
    w_on_left.wait_recv()
    w_mates.append(w_to_mate((g + 2) % 4, 9))
    w_mates[3].start()
    for copy in w_mates:
        copy.wait_recv()
    for copy in y_copies:
        copy.wait_recv()

    tokens = jnp.concatenate([x_all[i].astype(F32) for i in range(16)], axis=0).astype(BF16)
    for pair in range(2):
        y = jnp.zeros((128, 256), F32)
        for side in range(2):
            weight = jnp.concatenate([w_v[side, 2 * pair], w_v[side, 2 * pair + 1]], axis=1)
            y += jnp.dot(tokens[:, side * 512 : (side + 1) * 512], weight, preferred_element_type=F32)
        for i in range(16):
            e_o[i, :, pair * 256 : (pair + 1) * 256] = y[i * 8 : (i + 1) * 8].astype(BF16)

    e_copies = []
    for step in FAR_FIRST:
        for core in range(2):
            dest = ((x + step) % 8) * 2 + core
            e_copies.append(
                remote(
                    e_o.at[dest], er_o.at[step, c], e_send.at[step, core], e_recv.at[step, c], along_x(step, core)
                )
            )
    e_copies.append(remote(e_o.at[x * 2 + other], er_o.at[0, c], e_send.at[0, 0], e_recv.at[0, 0], mate))
    for copy in e_copies:
        copy.start()

    for copy in pair_copies + a_copies + y_copies + w_mates + list(d_copies.values()):
        copy.wait_send()
    for copy in (w_top_right, w_bottom_left, w_bottom_right, w_top_left, w_on_right, w_on_left):
        copy.wait_send()

    er_o[0, c] = e_o[t]
    for step in FAR_FIRST:
        for core in range(2):
            slot = er_o.at[step, core]
            remote(slot, slot, e_send.at[step, core], e_recv.at[step, core], along_x(step, core)).wait_recv()
    e_copies[-1].wait_recv()
    for copy in e_copies:
        copy.wait_send()
    result = []
    for core in range(2):
        summed = er_o[0, core].astype(F32)
        for step in range(1, 8):
            summed += er_o[step, core].astype(F32)
        result.append(summed)
    out_ref[...] = jnp.concatenate(result, axis=0).astype(BF16)


def on_device(queries, keys, values, cached_length, out_weight):
    hbm = pl.BlockSpec(memory_space=pl.ANY)
    dma = pltpu.SemaphoreType.DMA
    out = pl.pallas_call(
        kernel,
        out_shape=jax.ShapeDtypeStruct((16, 512), BF16),
        in_specs=[pl.BlockSpec(memory_space=pltpu.SMEM), hbm, hbm, hbm, hbm],
        out_specs=pl.BlockSpec(memory_space=pltpu.VMEM),
        scratch_shapes=[
            pltpu.VMEM((2, 2, 4, 8192), BF16),
            pltpu.VMEM((2, 2, 8, 128, 128), BF16),
            pltpu.VMEM((2, 2, 8, 128, 128), BF16),
            pltpu.VMEM((2, 4, 512, 128), BF16),
            pltpu.VMEM((8, 64, 128), BF16),
            pltpu.VMEM((8, 128), F32),
            pltpu.VMEM((8, 64, 128), BF16),
            pltpu.VMEM((8, 128), F32),
            pltpu.VMEM((8, 64, 128), F32),
            pltpu.VMEM((8, 128), F32),
            pltpu.VMEM((8, 64, 128), BF16),
            pltpu.VMEM((8, 1, 128), F32),
            pltpu.VMEM((8, 64, 128), BF16),
            pltpu.VMEM((8, 1, 128), F32),
            pltpu.VMEM((16, 8, 1024), BF16),
            pltpu.VMEM((16, 8, 512), BF16),
            pltpu.VMEM((8, 2, 8, 512), BF16),
            dma((2, 3)),
            dma,
            dma((2,)),
            dma((2,)),
            dma((10,)),
            dma((10,)),
            dma((8,)),
            dma((8,)),
            dma((8,)),
            dma((8,)),
            dma((8,)),
            dma((8,)),
            dma((8,)),
            dma((8,)),
            dma((8, 2)),
            dma((8, 2)),
        ],
        compiler_params=pltpu.CompilerParams(collective_id=0, has_side_effects=True),
        name="decode_step",
    )(cached_length, queries, keys, values, out_weight)
    return out.reshape(16, 4, 128)


def solution(mesh):
    in_specs = (
        P(("group", "dp"), None, None),
        P(("group", "dp"), None, "tensor", None),
        P(("group", "dp"), None, "tensor", None),
        P(("group", "dp")),
        P("tensor", ("group", "dp")),
    )
    out_specs = P(("group", "tensor"), None, "dp")
    return jax.shard_map(
        on_device, mesh=mesh, in_specs=in_specs, out_specs=out_specs, check_vma=False
    )
```

```python
import functools
import math

import jax
import jax.numpy as jnp
from jax import lax
from jax.experimental import pallas as pl
from jax.experimental.pallas import tpu as pltpu
from jax.sharding import PartitionSpec as P

MESH = pl.DeviceIdType.MESH
F32 = jnp.float32
BF16 = jnp.bfloat16
ORDER = (4, 3, 5, 2, 6, 1, 7, 0)


def remote(src, dst, send, recv, device):
    return pltpu.make_async_remote_copy(
        src_ref=src, dst_ref=dst, send_sem=send, recv_sem=recv, device_id=device, device_id_type=MESH
    )


def kernel(
    length_hbm,
    q_hbm,
    k_hbm,
    v_hbm,
    w_hbm,
    out_ref,
    length_ref,
    q_v,
    k_v,
    v_v,
    w_v,
    pair_o,
    pair_st,
    got_o,
    got_st,
    own_w,
    own_st,
    a_o,
    a_st,
    ar_o,
    ar_st,
    x_all,
    e_o,
    er_o,
    hello_sem,
    length_sem,
    load_sem,
    wload_sem,
    pair_send,
    pair_recv,
    w_send,
    w_recv,
    a_send,
    a_recv,
    ast_send,
    ast_recv,
    d_send,
    d_recv,
    e_send,
    e_recv,
):
    g = lax.axis_index("group")
    d = lax.axis_index("dp")
    t = lax.axis_index("tensor")
    x, c = t // 2, t % 2
    other = 1 - c
    ylo, z = d // 8, d % 8
    mate = {"tensor": x * 2 + other}
    right = {"group": (g + 1) % 4}
    left = {"group": (g + 3) % 4}

    def along_x(step, core):
        return {"tensor": ((x + step) % 8) * 2 + core}

    def plane(side, zz):
        return {"dp": (ylo if side == 0 else 1 - ylo) * 8 + zz}

    loads = []
    for slot, half in ((0, other), (1, c)):
        rows = pl.ds(half * 2, 2)
        for which, (src, dst) in enumerate(((q_hbm, q_v), (k_hbm, k_v), (v_hbm, v_v))):
            copy = pltpu.make_async_copy(src.at[rows], dst.at[slot], load_sem.at[slot, which])
            copy.start()
            loads.append(copy)
        if slot == 0:
            length_load = pltpu.make_async_copy(length_hbm, length_ref, length_sem)
            length_load.start()
    w_load = pltpu.make_async_copy(w_hbm, w_v.at[c, g], wload_sem)
    w_load.start()

    barrier = pltpu.get_barrier_semaphore()

    def greet(device):
        pl.semaphore_signal(barrier, inc=1, device_id=device, device_id_type=MESH)

    greet(mate)
    for step in range(1, 8):
        greet(along_x(step, 0))
        greet(along_x(step, 1))
    greet(plane(1, z))
    pl.when((g == 0) | (g == 1))(lambda: greet(right))
    pl.when((g == 0) | (g == 3))(lambda: greet(left))
    for zz in range(1, 8):

        @pl.when(zz > z)
        def _():
            greet(plane(0, zz))
            greet(plane(1, zz))

    lane = lax.broadcasted_iota(jnp.int32, (64, 128), 1)
    row = lax.broadcasted_iota(jnp.int32, (64, 128), 0)
    first_row = (row // 4) % 2 == 0
    low_eye = lane == row
    high_eye = lane == row + 64
    position = t * 128 + lane
    scale = 1.0 / math.sqrt(128)

    def attend(slot, step, allowed):
        k = (x + step) % 8
        features = pl.ds(pl.multiple_of(k * 1024, 1024), 1024)
        pair = jnp.concatenate([q_v[slot, r, :, features].astype(F32) for r in range(2)], axis=0)
        q = jnp.concatenate([pair[:, j * 128 : (j + 1) * 128] for j in range(8)], axis=0).astype(BF16)
        keys = jnp.concatenate([k_v[slot, 0, k].T, k_v[slot, 1, k].T], axis=1)
        vals = jnp.concatenate([v_v[slot, 0, k], v_v[slot, 1, k]], axis=0)
        s = jnp.dot(q, keys, preferred_element_type=F32)
        s = jnp.where(first_row, s[:, :128], s[:, 128:]) * scale
        s = jnp.where(allowed, s, -1e30)
        m = jnp.max(s, axis=1, keepdims=True)
        p = jnp.where(allowed, jnp.exp(s - m), 0.0)
        l = jnp.sum(p, axis=1, keepdims=True)
        both = jnp.concatenate(
            [jnp.where(first_row, p, 0.0), jnp.where(first_row, 0.0, p)], axis=1
        ).astype(BF16)
        w = jnp.dot(both, vals, preferred_element_type=F32)
        stats = jnp.where(low_eye, m, jnp.where(high_eye, l, 0.0))
        return w, jnp.sum(stats, axis=0, keepdims=True)

    def mask_of(half):
        horizon = jnp.where(first_row, length_ref[half * 2], length_ref[half * 2 + 1]) + row % 4 + 1
        return position < horizon

    def attend_other(chunk):
        done = [attend(0, ORDER[chunk * 4 + i], allowed) for i in range(4)]
        for i, (w, stats) in enumerate(done):
            pair_o[chunk, i] = w.astype(BF16)
        pair_st[chunk] = jnp.concatenate([stats for _, stats in done], axis=0)

    pair_copies = []

    def send_pair(chunk):
        for which, (src, dst) in enumerate(((pair_o, got_o), (pair_st, got_st))):
            copy = remote(
                src.at[chunk], dst.at[chunk], pair_send.at[chunk, which], pair_recv.at[chunk, which], mate
            )
            copy.start()
            pair_copies.append(copy)

    length_load.wait()
    for copy in loads[:3]:
        copy.wait()
    allowed = mask_of(other)
    attend_other(0)
    pl.semaphore_wait(barrier, 16 + (g % 2) + 2 * ((g // 2) * (1 - g % 2)) + 2 * z)
    send_pair(0)

    def hello(device):
        pl.semaphore_signal(hello_sem, inc=1, device_id=device, device_id_type=MESH)

    pl.when((g == 1) | (g == 2))(lambda: hello(left))
    pl.when((g == 2) | (g == 3))(lambda: hello(right))
    attend_other(1)
    send_pair(1)

    w_load.wait()
    top, bottom = pl.ds(0, 256), pl.ds(256, 256)

    def w_copy(block, part, index, device):
        ref = w_v.at[c, block, part]
        return remote(ref, ref, w_send.at[index], w_recv.at[index], device)

    w_top_right = w_copy(g, top, 0, right)
    w_bottom_left = w_copy(g, bottom, 1, left)
    w_bottom_right = w_copy(g, bottom, 2, right)
    w_top_left = w_copy(g, top, 3, left)

    def w_to_right():
        w_top_right.start()
        w_bottom_right.start()

    def w_to_left():
        w_bottom_left.start()
        w_top_left.start()

    def w_to_mate(block, index):
        ref = w_v.at[c, block]
        return remote(ref, ref, w_send.at[index], w_recv.at[index], mate)

    pl.when((g == 1) | (g == 2))(w_to_left)
    pl.when((g == 2) | (g == 3))(w_to_right)

    for copy in loads[3:]:
        copy.wait()
    allowed = mask_of(c)
    for chunk in range(2):
        done = [attend(1, ORDER[chunk * 4 + i], allowed) for i in range(4)]
        for i, (w, stats) in enumerate(done):
            own_w[chunk * 4 + i] = w
        own_st[chunk] = jnp.concatenate([stats for _, stats in done], axis=0)

    a_copies = []
    low = lax.broadcasted_iota(jnp.int32, (4, 128), 1) < 64
    for chunk in range(2):
        for copy in pair_copies[2 * chunk : 2 * chunk + 2]:
            copy.wait_recv()
        st1, st2 = own_st[chunk], got_st[chunk]
        top_both = jnp.maximum(st1, st2)
        e1, e2 = jnp.exp(st1 - top_both), jnp.exp(st2 - top_both)
        total = e1 * pltpu.roll(st1, 64, 1) + e2 * pltpu.roll(st2, 64, 1)
        merged = jnp.where(low, top_both, pltpu.roll(total, 64, 1))
        factors = jnp.where(low, e1, pltpu.roll(e2, 64, 1))
        for i in range(4):
            step = ORDER[chunk * 4 + i]
            f = factors[i : i + 1]
            f1 = jnp.sum(jnp.where(low_eye, f, 0.0), axis=1, keepdims=True)
            f2 = jnp.sum(jnp.where(high_eye, f, 0.0), axis=1, keepdims=True)
            a_o[step] = (f1 * own_w[chunk * 4 + i] + f2 * got_o[chunk, i].astype(F32)).astype(BF16)
            a_st[step] = merged[i : i + 1]
        for i in range(4):
            step = ORDER[chunk * 4 + i]
            if step == 0:
                continue
            to = along_x(step, c)
            pair = (
                remote(a_o.at[step], ar_o.at[step], a_send.at[step], a_recv.at[step], to),
                remote(a_st.at[step], ar_st.at[step], ast_send.at[step], ast_recv.at[step], to),
            )
            for copy in pair:
                copy.start()
                a_copies.append(copy)

    pl.when(g != 2)(lambda: pl.semaphore_wait(hello_sem, 2 - g % 2))
    pl.when((g == 0) | (g == 1))(w_to_right)
    pl.when((g == 0) | (g == 3))(w_to_left)
    w_mates = [w_to_mate(g, 6)]
    w_mates[0].start()
    w_on_right = w_copy((g + 3) % 4, top, 4, right)
    w_on_left = w_copy((g + 1) % 4, bottom, 5, left)

    def w_relay():
        w_top_right.wait_recv()
        w_on_right.start()
        w_bottom_left.wait_recv()
        w_on_left.start()

    pl.when(z < 4)(w_relay)

    for copy in a_copies:
        copy.wait_recv()
    st = jnp.concatenate([a_st[0]] + [ar_st[i] for i in range(1, 8)], axis=0)
    m = jnp.max(st, axis=0, keepdims=True)
    e = jnp.exp(st - m)
    total = jnp.sum(e * pltpu.roll(st, 64, 1), axis=0, keepdims=True)
    f = e / total
    attended = jnp.zeros((64, 128), F32)
    for i in range(8):
        part = a_o[0] if i == 0 else ar_o[i]
        fi = jnp.sum(jnp.where(low_eye, f[i : i + 1], 0.0), axis=1, keepdims=True)
        attended += fi * part.astype(F32)
    for j in range(8):
        x_all[d, :, j * 128 : (j + 1) * 128] = attended[j * 8 : (j + 1) * 8].astype(BF16)

    def d_copy(side, zz):
        ref = x_all.at[d]
        return remote(ref, ref, d_send.at[side, zz], d_recv.at[side, z], plane(side, zz))

    def d_arrival(side, zz):
        ref = x_all.at[d]
        return remote(ref, ref, d_send.at[side, zz], d_recv.at[side, zz], plane(side, z))

    def d_start(zz):
        d_copy(0, zz).start()
        d_copy(1, zz).start()

    @pl.when(z > 0)
    def _():
        d_start(0)
        d_copy(0, 0).wait_send()
        d_copy(1, 0).wait_send()

    for zz in (1, 2):
        pl.when(zz < z)(lambda: d_start(zz))
    d_copy(1, z).start()
    pl.when(z >= 4)(w_relay)
    for zz in (3, 4, 5, 6):
        pl.when(zz < z)(lambda: d_start(zz))
    w_bottom_right.wait_recv()
    w_mates.append(w_to_mate((g + 3) % 4, 7))
    w_mates[1].start()
    w_top_left.wait_recv()
    w_mates.append(w_to_mate((g + 1) % 4, 8))
    w_mates[2].start()

    def d_wait(zz):
        d_arrival(0, zz).wait_recv()
        d_arrival(1, zz).wait_recv()

    w_on_right.wait_recv()
    w_on_left.wait_recv()
    w_mates.append(w_to_mate((g + 2) % 4, 9))
    w_mates[3].start()
    for copy in w_mates:
        copy.wait_recv()

    def e_copy(block):
        return remote(
            e_o.at[block], er_o.at[t], e_send.at[block], e_recv.at[t], {"tensor": jnp.asarray(block, jnp.int32)}
        )

    last = z // 7
    for i in range(8):
        if i == 0:
            zz = z
        elif i == 1:
            zz = (1 - last) * (z + 1)
        else:
            zz = last * (i - 1) + (1 - last) * (i - 2 * ((z + 9 - i) // 8))
        if i == 0:
            d_arrival(1, zz).wait_recv()
        else:
            d_wait(zz)
            pl.when(zz > z)(lambda: d_start(zz))
        blocks = (ylo * 8 + zz, (1 - ylo) * 8 + zz)
        tokens = jnp.concatenate([x_all[block].astype(F32) for block in blocks], axis=0).astype(BF16)
        for pair in range(2):
            y = jnp.zeros((16, 256), F32)
            for side in range(2):
                weight = jnp.concatenate([w_v[side, 2 * pair], w_v[side, 2 * pair + 1]], axis=1)
                y += jnp.dot(tokens[:, side * 512 : (side + 1) * 512], weight, preferred_element_type=F32)
            for side in range(2):
                e_o[blocks[side], :, pair * 256 : (pair + 1) * 256] = y[side * 8 : (side + 1) * 8].astype(BF16)
        for block in blocks:
            pl.when(block != t)(lambda: e_copy(block).start())

    er_o[t] = e_o[t]
    for block in range(16):

        @pl.when(block != t)
        def _():
            ref = er_o.at[block]
            remote(ref, ref, e_send.at[block], e_recv.at[block], {"tensor": jnp.int32(block)}).wait_recv()

    result = []
    for core in range(2):
        summed = er_o[core].astype(F32)
        for step in range(1, 8):
            summed += er_o[2 * step + core].astype(F32)
        result.append(summed)
    out_ref[...] = jnp.concatenate(result, axis=0).astype(BF16)

    for copy in pair_copies + a_copies + w_mates:
        copy.wait_send()
    for copy in (w_top_right, w_bottom_left, w_bottom_right, w_top_left, w_on_right, w_on_left):
        copy.wait_send()
    for zz in range(1, 8):

        @pl.when(zz != z)
        def _():
            d_copy(0, zz).wait_send()
            d_copy(1, zz).wait_send()

    d_copy(1, z).wait_send()
    for block in range(16):

        @pl.when(block != t)
        def _():
            e_copy(block).wait_send()


def on_device(queries, keys, values, cached_length, out_weight):
    hbm = pl.BlockSpec(memory_space=pl.ANY)
    dma = pltpu.SemaphoreType.DMA
    out = pl.pallas_call(
        kernel,
        out_shape=jax.ShapeDtypeStruct((16, 512), BF16),
        in_specs=[hbm] * 5,
        out_specs=pl.BlockSpec(memory_space=pltpu.VMEM),
        scratch_shapes=[
            pltpu.SMEM((4,), jnp.int32),
            pltpu.VMEM((2, 2, 4, 8192), BF16),
            pltpu.VMEM((2, 2, 8, 128, 128), BF16),
            pltpu.VMEM((2, 2, 8, 128, 128), BF16),
            pltpu.VMEM((2, 4, 512, 128), BF16),
            pltpu.VMEM((2, 4, 64, 128), BF16),
            pltpu.VMEM((2, 4, 128), F32),
            pltpu.VMEM((2, 4, 64, 128), BF16),
            pltpu.VMEM((2, 4, 128), F32),
            pltpu.VMEM((8, 64, 128), F32),
            pltpu.VMEM((2, 4, 128), F32),
            pltpu.VMEM((8, 64, 128), BF16),
            pltpu.VMEM((8, 1, 128), F32),
            pltpu.VMEM((8, 64, 128), BF16),
            pltpu.VMEM((8, 1, 128), F32),
            pltpu.VMEM((16, 8, 1024), BF16),
            pltpu.VMEM((16, 8, 512), BF16),
            pltpu.VMEM((16, 8, 512), BF16),
            pltpu.SemaphoreType.REGULAR,
            dma,
            dma((2, 3)),
            dma,
            dma((2, 2)),
            dma((2, 2)),
            dma((10,)),
            dma((10,)),
            dma((8,)),
            dma((8,)),
            dma((8,)),
            dma((8,)),
            dma((2, 8)),
            dma((2, 8)),
            dma((16,)),
            dma((16,)),
        ],
        compiler_params=pltpu.CompilerParams(collective_id=0, has_side_effects=True),
        name="decode_step",
    )(cached_length, queries, keys, values, out_weight)
    return out.reshape(16, 4, 128)


def solution(mesh):
    in_specs = (
        P(("group", "dp"), None, None),
        P(("group", "dp"), None, "tensor", None),
        P(("group", "dp"), None, "tensor", None),
        P(("group", "dp")),
        P("tensor", ("group", "dp")),
    )
    out_specs = P(("group", "tensor"), None, "dp")
    return jax.shard_map(
        on_device, mesh=mesh, in_specs=in_specs, out_specs=out_specs, check_vma=False
    )
```

```python
import functools
import math

import jax
import jax.numpy as jnp
from jax import lax
from jax.experimental import pallas as pl
from jax.experimental.pallas import tpu as pltpu
from jax.sharding import PartitionSpec as P

MESH = pl.DeviceIdType.MESH
F32 = jnp.float32
BF16 = jnp.bfloat16
ORDER = (4, 3, 5, 2, 6, 1, 7, 0)


def remote(src, dst, send, recv, device):
    return pltpu.make_async_remote_copy(
        src_ref=src, dst_ref=dst, send_sem=send, recv_sem=recv, device_id=device, device_id_type=MESH
    )


def kernel(
    length_hbm,
    q_hbm,
    k_hbm,
    v_hbm,
    w_hbm,
    out_ref,
    length_ref,
    q_v,
    k_v,
    v_v,
    w_v,
    pair_o,
    pair_st,
    got_o,
    got_st,
    own_w,
    own_st,
    a_o,
    a_st,
    ar_o,
    ar_st,
    x_all,
    e_o,
    er_o,
    hello_sem,
    hello_x_sem,
    length_sem,
    load_sem,
    wload_sem,
    pair_send,
    pair_recv,
    w_send,
    w_recv,
    a_send,
    a_recv,
    ast_send,
    ast_recv,
    d_send,
    d_recv,
    e_send,
    e_recv,
):
    g = lax.axis_index("group")
    d = lax.axis_index("dp")
    t = lax.axis_index("tensor")
    x, c = t // 2, t % 2
    other = 1 - c
    ylo, z = d // 8, d % 8
    mate = {"tensor": x * 2 + other}
    right = {"group": (g + 1) % 4}
    left = {"group": (g + 3) % 4}

    def along_x(step, core):
        return {"tensor": ((x + step) % 8) * 2 + core}

    def plane(side, zz):
        return {"dp": (ylo if side == 0 else 1 - ylo) * 8 + zz}

    loads = []
    for slot, half in ((0, other), (1, c)):
        rows = pl.ds(half * 2, 2)
        for which, (src, dst) in enumerate(((q_hbm, q_v), (k_hbm, k_v), (v_hbm, v_v))):
            copy = pltpu.make_async_copy(src.at[rows], dst.at[slot], load_sem.at[slot, which])
            copy.start()
            loads.append(copy)
        if slot == 0:
            length_load = pltpu.make_async_copy(length_hbm, length_ref, length_sem)
            length_load.start()
    w_load = pltpu.make_async_copy(w_hbm, w_v.at[c, g], wload_sem)
    w_load.start()

    barrier = pltpu.get_barrier_semaphore()

    def greet(device):
        pl.semaphore_signal(barrier, inc=1, device_id=device, device_id_type=MESH)

    def rank_of(v):
        return v - 2 * (v // 5) * (v - 4)

    def along_x_if(test, act):
        for step in range(1, 8):

            @pl.when(test(rank_of((x + step) % 8), rank))
            def _():
                act(along_x(step, 0))
                act(along_x(step, 1))

    rank = rank_of(x)
    greet(mate)
    greet(plane(1, z))
    along_x_if(lambda theirs, mine: theirs >= mine, greet)
    pl.when((g == 0) | (g == 1))(lambda: greet(right))
    pl.when((g == 0) | (g == 3))(lambda: greet(left))
    for zz in range(1, 8):

        @pl.when(zz > z)
        def _():
            greet(plane(0, zz))
            greet(plane(1, zz))

    lane = lax.broadcasted_iota(jnp.int32, (64, 128), 1)
    row = lax.broadcasted_iota(jnp.int32, (64, 128), 0)
    first_row = (row // 4) % 2 == 0
    low_eye = lane == row
    high_eye = lane == row + 64
    position = t * 128 + lane
    scale = 1.0 / math.sqrt(128)

    def attend(slot, step, allowed):
        k = (x + step) % 8
        features = pl.ds(pl.multiple_of(k * 1024, 1024), 1024)
        pair = jnp.concatenate([q_v[slot, r, :, features].astype(F32) for r in range(2)], axis=0)
        q = jnp.concatenate([pair[:, j * 128 : (j + 1) * 128] for j in range(8)], axis=0).astype(BF16)
        keys = jnp.concatenate([k_v[slot, 0, k].T, k_v[slot, 1, k].T], axis=1)
        vals = jnp.concatenate([v_v[slot, 0, k], v_v[slot, 1, k]], axis=0)
        s = jnp.dot(q, keys, preferred_element_type=F32)
        s = jnp.where(first_row, s[:, :128], s[:, 128:]) * scale
        s = jnp.where(allowed, s, -1e30)
        m = jnp.max(s, axis=1, keepdims=True)
        p = jnp.where(allowed, jnp.exp(s - m), 0.0)
        l = jnp.sum(p, axis=1, keepdims=True)
        both = jnp.concatenate(
            [jnp.where(first_row, p, 0.0), jnp.where(first_row, 0.0, p)], axis=1
        ).astype(BF16)
        w = jnp.dot(both, vals, preferred_element_type=F32)
        stats = jnp.where(low_eye, m, jnp.where(high_eye, l, 0.0))
        return w, jnp.sum(stats, axis=0, keepdims=True)

    def mask_of(half):
        horizon = jnp.where(first_row, length_ref[half * 2], length_ref[half * 2 + 1]) + row % 4 + 1
        return position < horizon

    def attend_other(chunk):
        done = [attend(0, ORDER[chunk * 4 + i], allowed) for i in range(4)]
        for i, (w, stats) in enumerate(done):
            pair_o[chunk, i] = w.astype(BF16)
        pair_st[chunk] = jnp.concatenate([stats for _, stats in done], axis=0)

    pair_copies = []

    def send_pair(chunk):
        for which, (src, dst) in enumerate(((pair_o, got_o), (pair_st, got_st))):
            copy = remote(
                src.at[chunk], dst.at[chunk], pair_send.at[which], pair_recv.at[chunk, which], mate
            )
            copy.start()
            pair_copies.append(copy)

    before_x = 4 * rank - 2 * (rank // 4)
    pl.semaphore_wait(barrier, 2 + before_x + (g % 2) + 2 * ((g // 2) * (1 - g % 2)) + 2 * z)

    def hello(sem, device):
        pl.semaphore_signal(sem, inc=1, device_id=device, device_id_type=MESH)

    along_x_if(lambda theirs, mine: theirs < mine, lambda device: hello(hello_x_sem, device))
    pl.when((g == 1) | (g == 2))(lambda: hello(hello_sem, left))
    pl.when((g == 2) | (g == 3))(lambda: hello(hello_sem, right))

    length_load.wait()
    for copy in loads[:3]:
        copy.wait()
    allowed = mask_of(other)
    attend_other(0)
    send_pair(0)
    attend_other(1)
    send_pair(1)

    w_load.wait()
    top, bottom = pl.ds(0, 256), pl.ds(256, 256)

    def w_copy(block, part, index, device):
        ref = w_v.at[c, block, part]
        return remote(ref, ref, w_send.at[0], w_recv.at[index], device)

    w_top_right = w_copy(g, top, 0, right)
    w_bottom_left = w_copy(g, bottom, 1, left)
    w_bottom_right = w_copy(g, bottom, 2, right)
    w_top_left = w_copy(g, top, 3, left)

    def w_to_right():
        w_top_right.start()
        w_bottom_right.start()

    def w_to_left():
        w_bottom_left.start()
        w_top_left.start()

    def w_to_mate(block):
        ref = w_v.at[c, block]
        remote(ref, ref, w_send.at[1], w_recv.at[6], mate).start()

    pl.when((g == 1) | (g == 2))(w_to_left)
    pl.when((g == 2) | (g == 3))(w_to_right)

    for copy in loads[3:]:
        copy.wait()
    allowed = mask_of(c)
    for chunk in range(2):
        done = [attend(1, ORDER[chunk * 4 + i], allowed) for i in range(4)]
        for i, (w, stats) in enumerate(done):
            own_w[chunk * 4 + i] = w
        own_st[chunk] = jnp.concatenate([stats for _, stats in done], axis=0)

    a_copies = (
        remote(ar_o.at[pl.ds(1, 7)], ar_o.at[pl.ds(1, 7)], a_send, a_recv, mate),
        remote(ar_st.at[pl.ds(1, 7)], ar_st.at[pl.ds(1, 7)], ast_send, ast_recv, mate),
    )
    low = lax.broadcasted_iota(jnp.int32, (4, 128), 1) < 64
    for chunk in range(2):
        for copy in pair_copies[2 * chunk : 2 * chunk + 2]:
            copy.wait_recv()
        st1, st2 = own_st[chunk], got_st[chunk]
        top_both = jnp.maximum(st1, st2)
        e1, e2 = jnp.exp(st1 - top_both), jnp.exp(st2 - top_both)
        total = e1 * pltpu.roll(st1, 64, 1) + e2 * pltpu.roll(st2, 64, 1)
        merged = jnp.where(low, top_both, pltpu.roll(total, 64, 1))
        factors = jnp.where(low, e1, pltpu.roll(e2, 64, 1))
        for i in range(4):
            step = ORDER[chunk * 4 + i]
            f = factors[i : i + 1]
            f1 = jnp.sum(jnp.where(low_eye, f, 0.0), axis=1, keepdims=True)
            f2 = jnp.sum(jnp.where(high_eye, f, 0.0), axis=1, keepdims=True)
            a_o[step] = (f1 * own_w[chunk * 4 + i] + f2 * got_o[chunk, i].astype(F32)).astype(BF16)
            a_st[step] = merged[i : i + 1]
        if chunk == 0:
            pl.when(rank < 4)(lambda: pl.semaphore_wait(hello_x_sem, 14 - before_x))
        for i in range(4):
            step = ORDER[chunk * 4 + i]
            if step == 0:
                continue
            to = along_x(step, c)
            pair = (
                remote(a_o.at[step], ar_o.at[step], a_send, a_recv, to),
                remote(a_st.at[step], ar_st.at[step], ast_send, ast_recv, to),
            )
            for copy in pair:
                copy.start()

    pl.when(g != 2)(lambda: pl.semaphore_wait(hello_sem, 2 - g % 2))
    to_right, to_left = (g == 0) | (g == 1), (g == 0) | (g == 3)
    pl.when(to_right)(lambda: w_top_right.start())
    pl.when(to_left)(lambda: w_bottom_left.start())
    pl.when(to_right & (z < 4))(lambda: w_bottom_right.start())
    pl.when(to_left & (z < 4))(lambda: w_top_left.start())
    w_to_mate(g)
    w_on_right = w_copy((g + 3) % 4, top, 4, right)
    w_on_left = w_copy((g + 1) % 4, bottom, 5, left)

    def w_relay():
        w_top_right.wait_recv()
        w_on_right.start()
        w_bottom_left.wait_recv()
        w_on_left.start()

    pl.when(z < 4)(w_relay)

    for copy in a_copies:
        copy.wait_recv()
    st = jnp.concatenate([a_st[0]] + [ar_st[i] for i in range(1, 8)], axis=0)
    m = jnp.max(st, axis=0, keepdims=True)
    e = jnp.exp(st - m)
    total = jnp.sum(e * pltpu.roll(st, 64, 1), axis=0, keepdims=True)
    f = e / total
    attended = jnp.zeros((64, 128), F32)
    for i in range(8):
        part = a_o[0] if i == 0 else ar_o[i]
        fi = jnp.sum(jnp.where(low_eye, f[i : i + 1], 0.0), axis=1, keepdims=True)
        attended += fi * part.astype(F32)
    for j in range(8):
        x_all[d, :, j * 128 : (j + 1) * 128] = attended[j * 8 : (j + 1) * 8].astype(BF16)

    def d_copy(side, zz):
        ref = x_all.at[d]
        return remote(ref, ref, d_send, d_recv.at[z], plane(side, zz))

    def d_arrival(count, zz):
        ref = x_all.at[pl.ds(0, count)]
        return remote(ref, ref, d_send, d_recv.at[zz], plane(1, z))

    def d_start(zz):
        d_copy(0, zz).start()
        d_copy(1, zz).start()

    for zz in (0, 1, 2, 3):
        pl.when(zz < z)(lambda: d_start(zz))
    d_copy(1, z).start()
    pl.when(to_right & (z >= 4))(lambda: w_bottom_right.start())
    pl.when(to_left & (z >= 4))(lambda: w_top_left.start())
    pl.when(z >= 4)(w_relay)
    for zz in (4, 5, 6):
        pl.when(zz < z)(lambda: d_start(zz))
    w_bottom_right.wait_recv()
    w_to_mate((g + 3) % 4)
    w_top_left.wait_recv()
    w_to_mate((g + 1) % 4)

    def d_wait(zz):
        d_arrival(2, zz).wait_recv()

    for zz in (5, 6, 7):

        @pl.when((z >= 4) & (zz > z))
        def _():
            d_wait(zz)
            d_start(zz)

    w_on_right.wait_recv()
    w_on_left.wait_recv()
    w_to_mate((g + 2) % 4)
    remote(w_v.at[other], w_v.at[other], w_send.at[1], w_recv.at[6], mate).wait_recv()

    def e_copy(block):
        return remote(
            e_o.at[block], er_o.at[t], e_send, e_recv, {"tensor": jnp.asarray(block, jnp.int32)}
        )

    last = z // 7
    for i in range(8):
        if i == 0:
            zz = z
        elif i == 1:
            zz = (1 - last) * (z + 1)
        else:
            zz = last * (i - 1) + (1 - last) * (i - 2 * ((z + 9 - i) // 8))
        if i == 0:
            d_arrival(1, zz).wait_recv()
        else:
            pl.when((zz < z) | (z < 4))(lambda: d_wait(zz))
            pl.when((zz > z) & (z < 4))(lambda: d_start(zz))
        blocks = (ylo * 8 + zz, (1 - ylo) * 8 + zz)
        tokens = jnp.concatenate([x_all[block].astype(F32) for block in blocks], axis=0).astype(BF16)
        for pair in range(2):
            y = jnp.zeros((16, 256), F32)
            for side in range(2):
                weight = jnp.concatenate([w_v[side, 2 * pair], w_v[side, 2 * pair + 1]], axis=1)
                y += jnp.dot(tokens[:, side * 512 : (side + 1) * 512], weight, preferred_element_type=F32)
            for side in range(2):
                e_o[blocks[side], :, pair * 256 : (pair + 1) * 256] = y[side * 8 : (side + 1) * 8].astype(BF16)
        for block in blocks:
            pl.when(block != t)(lambda: e_copy(block).start())

    er_o[t] = e_o[t]
    others_e = er_o.at[pl.ds(0, 15)]
    remote(others_e, others_e, e_send, e_recv, mate).wait_recv()

    result = []
    for core in range(2):
        summed = er_o[core].astype(F32)
        for step in range(1, 8):
            summed += er_o[2 * step + core].astype(F32)
        result.append(summed)
    out_ref[...] = jnp.concatenate(result, axis=0).astype(BF16)

    for which, ref in enumerate((pair_o, pair_st)):
        remote(ref, ref, pair_send.at[which], pair_recv.at[0, which], mate).wait_send()
    for copy in a_copies:
        copy.wait_send()
    for which, count in enumerate((3, 4)):
        ref = w_v.at[c, pl.ds(0, count)]
        remote(ref, ref, w_send.at[which], w_recv.at[6], mate).wait_send()
    all_x = x_all.at[pl.ds(0, 15)]
    remote(all_x, all_x, d_send, d_recv.at[z], mate).wait_send()
    remote(others_e, others_e, e_send, e_recv, mate).wait_send()


def on_device(queries, keys, values, cached_length, out_weight):
    hbm = pl.BlockSpec(memory_space=pl.ANY)
    dma = pltpu.SemaphoreType.DMA
    out = pl.pallas_call(
        kernel,
        out_shape=pltpu.VMEM((16, 512), BF16),
        in_specs=[hbm] * 5,
        out_specs=pl.BlockSpec(memory_space=pltpu.VMEM),
        scratch_shapes=[
            pltpu.SMEM((4,), jnp.int32),
            pltpu.VMEM((2, 2, 4, 8192), BF16),
            pltpu.VMEM((2, 2, 8, 128, 128), BF16),
            pltpu.VMEM((2, 2, 8, 128, 128), BF16),
            pltpu.VMEM((2, 4, 512, 128), BF16),
            pltpu.VMEM((2, 4, 64, 128), BF16),
            pltpu.VMEM((2, 4, 128), F32),
            pltpu.VMEM((2, 4, 64, 128), BF16),
            pltpu.VMEM((2, 4, 128), F32),
            pltpu.VMEM((8, 64, 128), F32),
            pltpu.VMEM((2, 4, 128), F32),
            pltpu.VMEM((8, 64, 128), BF16),
            pltpu.VMEM((8, 1, 128), F32),
            pltpu.VMEM((8, 64, 128), BF16),
            pltpu.VMEM((8, 1, 128), F32),
            pltpu.VMEM((16, 8, 1024), BF16),
            pltpu.VMEM((16, 8, 512), BF16),
            pltpu.VMEM((16, 8, 512), BF16),
            pltpu.SemaphoreType.REGULAR,
            pltpu.SemaphoreType.REGULAR,
            dma,
            dma((2, 3)),
            dma,
            dma((2,)),
            dma((2, 2)),
            dma((2,)),
            dma((7,)),
            dma,
            dma,
            dma,
            dma,
            dma,
            dma((8,)),
            dma,
            dma,
        ],
        compiler_params=pltpu.CompilerParams(collective_id=0, has_side_effects=True),
        name="decode_step",
    )(cached_length, queries, keys, values, out_weight)
    return out.reshape(16, 4, 128)


def solution(mesh):
    in_specs = (
        P(("group", "dp"), None, None),
        P(("group", "dp"), None, "tensor", None),
        P(("group", "dp"), None, "tensor", None),
        P(("group", "dp")),
        P("tensor", ("group", "dp")),
    )
    out_specs = P(("group", "tensor"), None, "dp")
    return jax.shard_map(
        on_device, mesh=mesh, in_specs=in_specs, out_specs=out_specs, check_vma=False
    )
```

```python
import functools
import math

import jax
import jax.numpy as jnp
from jax import lax
from jax.experimental import pallas as pl
from jax.experimental.pallas import tpu as pltpu
from jax.sharding import PartitionSpec as P

MESH = pl.DeviceIdType.MESH
F32 = jnp.float32
BF16 = jnp.bfloat16
ORDER = (4, 3, 5, 2, 6, 1, 7, 0)


def remote(src, dst, send, recv, device):
    return pltpu.make_async_remote_copy(
        src_ref=src, dst_ref=dst, send_sem=send, recv_sem=recv, device_id=device, device_id_type=MESH
    )


def kernel(
    length_hbm,
    q_hbm,
    k_hbm,
    v_hbm,
    w_hbm,
    out_ref,
    length_ref,
    q_v,
    k_v,
    v_v,
    w_v,
    pair_o,
    pair_st,
    got_o,
    got_st,
    own_w,
    own_st,
    a_o,
    a_st,
    ar_o,
    ar_st,
    x_all,
    e_o,
    er_o,
    hello_sem,
    hello_x_sem,
    length_sem,
    load_sem,
    wload_sem,
    pair_send,
    pair_recv,
    w_send,
    w_recv,
    a_send,
    a_recv,
    ast_send,
    ast_recv,
    d_send,
    d_recv,
    e_send,
    e_recv,
):
    g = lax.axis_index("group")
    d = lax.axis_index("dp")
    t = lax.axis_index("tensor")
    x, c = t // 2, t % 2
    other = 1 - c
    ylo, z = d // 8, d % 8
    mate = {"tensor": x * 2 + other}
    right = {"group": (g + 1) % 4}
    left = {"group": (g + 3) % 4}

    def along_x(step, core):
        return {"tensor": ((x + step) % 8) * 2 + core}

    def plane(side, zz):
        return {"dp": (ylo if side == 0 else 1 - ylo) * 8 + zz}

    loads = []
    for slot, half in ((0, other), (1, c)):
        rows = pl.ds(half * 2, 2)
        for which, (src, dst) in enumerate(((q_hbm, q_v), (k_hbm, k_v), (v_hbm, v_v))):
            copy = pltpu.make_async_copy(src.at[rows], dst.at[slot], load_sem.at[slot, which])
            copy.start()
            loads.append(copy)
        if slot == 0:
            length_load = pltpu.make_async_copy(length_hbm, length_ref, length_sem)
            length_load.start()
    w_load = pltpu.make_async_copy(w_hbm, w_v.at[c, g], wload_sem)
    w_load.start()

    barrier = pltpu.get_barrier_semaphore()

    def greet(device):
        pl.semaphore_signal(barrier, inc=1, device_id=device, device_id_type=MESH)

    def rank_of(v):
        return v - 2 * (v // 5) * (v - 4)

    def along_x_if(test, act):
        for step in range(1, 8):

            @pl.when(test(rank_of((x + step) % 8), rank))
            def _():
                act(along_x(step, 0))
                act(along_x(step, 1))

    rank = rank_of(x)
    greet(mate)
    greet(plane(1, z))
    along_x_if(lambda theirs, mine: theirs >= mine, greet)
    pl.when((g == 0) | (g == 1))(lambda: greet(right))
    pl.when((g == 0) | (g == 3))(lambda: greet(left))
    for zz in range(1, 8):

        @pl.when(zz > z)
        def _():
            greet(plane(0, zz))
            greet(plane(1, zz))

    lane = lax.broadcasted_iota(jnp.int32, (64, 128), 1)
    row = lax.broadcasted_iota(jnp.int32, (64, 128), 0)
    first_row = (row // 4) % 2 == 0
    low_eye = lane == row
    high_eye = lane == row + 64
    position = t * 128 + lane
    scale = 1.0 / math.sqrt(128)

    def attend(slot, step, allowed):
        k = (x + step) % 8
        features = pl.ds(pl.multiple_of(k * 1024, 1024), 1024)
        pair = jnp.concatenate([q_v[slot, r, :, features].astype(F32) for r in range(2)], axis=0)
        q = jnp.concatenate([pair[:, j * 128 : (j + 1) * 128] for j in range(8)], axis=0).astype(BF16)
        keys = jnp.concatenate([k_v[slot, 0, k].T, k_v[slot, 1, k].T], axis=1)
        vals = jnp.concatenate([v_v[slot, 0, k], v_v[slot, 1, k]], axis=0)
        s = jnp.dot(q, keys, preferred_element_type=F32)
        s = jnp.where(first_row, s[:, :128], s[:, 128:]) * scale
        s = jnp.where(allowed, s, -1e30)
        m = jnp.max(s, axis=1, keepdims=True)
        p = jnp.where(allowed, jnp.exp(s - m), 0.0)
        l = jnp.sum(p, axis=1, keepdims=True)
        both = jnp.concatenate(
            [jnp.where(first_row, p, 0.0), jnp.where(first_row, 0.0, p)], axis=1
        ).astype(BF16)
        w = jnp.dot(both, vals, preferred_element_type=F32)
        stats = jnp.where(low_eye, m, jnp.where(high_eye, l, 0.0))
        return w, jnp.sum(stats, axis=0, keepdims=True)

    def mask_of(half):
        horizon = jnp.where(first_row, length_ref[half * 2], length_ref[half * 2 + 1]) + row % 4 + 1
        return position < horizon

    def attend_other(chunk):
        done = [attend(0, ORDER[chunk * 4 + i], allowed) for i in range(4)]
        for i, (w, stats) in enumerate(done):
            pair_o[chunk, i] = w.astype(BF16)
        pair_st[chunk] = jnp.concatenate([stats for _, stats in done], axis=0)

    pair_copies = []

    def send_pair(chunk):
        for which, (src, dst) in enumerate(((pair_o, got_o), (pair_st, got_st))):
            copy = remote(
                src.at[chunk], dst.at[chunk], pair_send.at[which], pair_recv.at[chunk, which], mate
            )
            copy.start()
            pair_copies.append(copy)

    before_x = 4 * rank - 2 * (rank // 4)
    pl.semaphore_wait(barrier, 2 + before_x + (g % 2) + 2 * ((g // 2) * (1 - g % 2)) + 2 * z)

    def hello(sem, device):
        pl.semaphore_signal(sem, inc=1, device_id=device, device_id_type=MESH)

    along_x_if(lambda theirs, mine: theirs < mine, lambda device: hello(hello_x_sem, device))
    pl.when((g == 1) | (g == 2))(lambda: hello(hello_sem, left))
    pl.when((g == 2) | (g == 3))(lambda: hello(hello_sem, right))

    length_load.wait()
    for copy in loads[:3]:
        copy.wait()
    allowed = mask_of(other)
    attend_other(0)
    send_pair(0)
    attend_other(1)
    send_pair(1)

    w_load.wait()
    top, bottom = pl.ds(0, 256), pl.ds(256, 256)

    def w_copy(block, part, index, device):
        ref = w_v.at[c, block, part]
        return remote(ref, ref, w_send.at[0], w_recv.at[index], device)

    w_top_right = w_copy(g, top, 0, right)
    w_bottom_left = w_copy(g, bottom, 1, left)
    w_bottom_right = w_copy(g, bottom, 2, right)
    w_top_left = w_copy(g, top, 3, left)

    def w_to_right():
        w_top_right.start()
        w_bottom_right.start()

    def w_to_left():
        w_bottom_left.start()
        w_top_left.start()

    def w_to_mate(block):
        ref = w_v.at[c, block]
        remote(ref, ref, w_send.at[1], w_recv.at[6], mate).start()

    pl.when((g == 1) | (g == 2))(w_to_left)
    pl.when((g == 2) | (g == 3))(w_to_right)

    for copy in loads[3:]:
        copy.wait()
    allowed = mask_of(c)
    for chunk in range(2):
        done = [attend(1, ORDER[chunk * 4 + i], allowed) for i in range(4)]
        for i, (w, stats) in enumerate(done):
            own_w[chunk * 4 + i] = w
        own_st[chunk] = jnp.concatenate([stats for _, stats in done], axis=0)

    a_copies = (
        remote(ar_o.at[pl.ds(1, 7)], ar_o.at[pl.ds(1, 7)], a_send, a_recv, mate),
        remote(ar_st.at[pl.ds(1, 7)], ar_st.at[pl.ds(1, 7)], ast_send, ast_recv, mate),
    )
    low = lax.broadcasted_iota(jnp.int32, (4, 128), 1) < 64
    for chunk in range(2):
        for copy in pair_copies[2 * chunk : 2 * chunk + 2]:
            copy.wait_recv()
        st1, st2 = own_st[chunk], got_st[chunk]
        top_both = jnp.maximum(st1, st2)
        e1, e2 = jnp.exp(st1 - top_both), jnp.exp(st2 - top_both)
        total = e1 * pltpu.roll(st1, 64, 1) + e2 * pltpu.roll(st2, 64, 1)
        merged = jnp.where(low, top_both, pltpu.roll(total, 64, 1))
        factors = jnp.where(low, e1, pltpu.roll(e2, 64, 1))
        for i in range(4):
            step = ORDER[chunk * 4 + i]
            f = factors[i : i + 1]
            f1 = jnp.sum(jnp.where(low_eye, f, 0.0), axis=1, keepdims=True)
            f2 = jnp.sum(jnp.where(high_eye, f, 0.0), axis=1, keepdims=True)
            a_o[step] = (f1 * own_w[chunk * 4 + i] + f2 * got_o[chunk, i].astype(F32)).astype(BF16)
            a_st[step] = merged[i : i + 1]
        if chunk == 0:
            pl.when(rank < 4)(lambda: pl.semaphore_wait(hello_x_sem, 14 - before_x))
        for i in range(4):
            step = ORDER[chunk * 4 + i]
            if step == 0:
                continue
            to = along_x(step, c)
            pair = (
                remote(a_o.at[step], ar_o.at[step], a_send, a_recv, to),
                remote(a_st.at[step], ar_st.at[step], ast_send, ast_recv, to),
            )
            for copy in pair:
                copy.start()

    pl.when(g != 2)(lambda: pl.semaphore_wait(hello_sem, 2 - g % 2))
    to_right, to_left = (g == 0) | (g == 1), (g == 0) | (g == 3)
    pl.when(to_right)(lambda: w_top_right.start())
    pl.when(to_left)(lambda: w_bottom_left.start())
    pl.when(to_right & (z < 4))(lambda: w_bottom_right.start())
    pl.when(to_left & (z < 4))(lambda: w_top_left.start())
    w_to_mate(g)
    w_on_right = w_copy((g + 3) % 4, top, 4, right)
    w_on_left = w_copy((g + 1) % 4, bottom, 5, left)

    def w_relay():
        w_top_right.wait_recv()
        w_on_right.start()
        w_bottom_left.wait_recv()
        w_on_left.start()

    pl.when(z < 4)(w_relay)

    for copy in a_copies:
        copy.wait_recv()
    st = jnp.concatenate([a_st[0]] + [ar_st[i] for i in range(1, 8)], axis=0)
    m = jnp.max(st, axis=0, keepdims=True)
    e = jnp.exp(st - m)
    total = jnp.sum(e * pltpu.roll(st, 64, 1), axis=0, keepdims=True)
    f = e / total
    attended = jnp.zeros((64, 128), F32)
    for i in range(8):
        part = a_o[0] if i == 0 else ar_o[i]
        fi = jnp.sum(jnp.where(low_eye, f[i : i + 1], 0.0), axis=1, keepdims=True)
        attended += fi * part.astype(F32)
    for j in range(8):
        x_all[d, :, j * 128 : (j + 1) * 128] = attended[j * 8 : (j + 1) * 8].astype(BF16)

    def d_copy(side, zz):
        ref = x_all.at[d]
        first = isinstance(zz, int) and zz == 0
        return remote(ref, ref, d_send.at[0 if first else 1], d_recv.at[z], plane(side, zz))

    def d_arrival(count, zz):
        ref = x_all.at[pl.ds(0, count)]
        return remote(ref, ref, d_send.at[1], d_recv.at[zz], plane(1, z))

    def d_start(zz):
        d_copy(1, zz).start()
        d_copy(0, zz).start()

    for zz in (0, 1, 3):
        pl.when(zz < z)(lambda: d_start(zz))

    @pl.when(z > 0)
    def _():
        two = x_all.at[pl.ds(0, 2)]
        remote(two, two, d_send.at[0], d_recv.at[z], mate).wait_send()

    pl.when(2 < z)(lambda: d_start(2))
    d_copy(1, z).start()
    pl.when(to_right & (z >= 4))(lambda: w_bottom_right.start())
    pl.when(to_left & (z >= 4))(lambda: w_top_left.start())
    pl.when(z >= 4)(w_relay)
    for zz in (4, 5, 6):
        pl.when(zz < z)(lambda: d_start(zz))
    w_bottom_right.wait_recv()
    w_to_mate((g + 3) % 4)
    w_top_left.wait_recv()
    w_to_mate((g + 1) % 4)

    def d_wait(zz):
        d_arrival(2, zz).wait_recv()

    for zz in (5, 6, 7):

        @pl.when((z >= 4) & (zz > z))
        def _():
            d_wait(zz)
            d_start(zz)

    w_on_right.wait_recv()
    w_on_left.wait_recv()
    w_to_mate((g + 2) % 4)
    remote(w_v.at[other], w_v.at[other], w_send.at[1], w_recv.at[6], mate).wait_recv()

    def e_copy(block):
        return remote(
            e_o.at[block], er_o.at[t], e_send, e_recv, {"tensor": jnp.asarray(block, jnp.int32)}
        )

    last = z // 7
    for i in range(8):
        if i == 0:
            zz = z
        elif i == 1:
            zz = (1 - last) * (z + 1)
        else:
            zz = last * (i - 1) + (1 - last) * (i - 2 * ((z + 9 - i) // 8))
        if i == 0:
            d_arrival(1, zz).wait_recv()
        else:
            pl.when((zz < z) | (z < 4))(lambda: d_wait(zz))
            pl.when((zz > z) & (z < 4))(lambda: d_start(zz))
        blocks = (ylo * 8 + zz, (1 - ylo) * 8 + zz)
        tokens = jnp.concatenate([x_all[block].astype(F32) for block in blocks], axis=0).astype(BF16)
        for pair in range(2):
            y = jnp.zeros((16, 256), F32)
            for side in range(2):
                weight = jnp.concatenate([w_v[side, 2 * pair], w_v[side, 2 * pair + 1]], axis=1)
                y += jnp.dot(tokens[:, side * 512 : (side + 1) * 512], weight, preferred_element_type=F32)
            for side in range(2):
                e_o[blocks[side], :, pair * 256 : (pair + 1) * 256] = y[side * 8 : (side + 1) * 8].astype(BF16)
        for block in blocks:
            pl.when(block != t)(lambda: e_copy(block).start())

    er_o[t] = e_o[t]
    others_e = er_o.at[pl.ds(0, 15)]
    remote(others_e, others_e, e_send, e_recv, mate).wait_recv()

    result = []
    for core in range(2):
        summed = er_o[core].astype(F32)
        for step in range(1, 8):
            summed += er_o[2 * step + core].astype(F32)
        result.append(summed)
    out_ref[...] = jnp.concatenate(result, axis=0).astype(BF16)

    for which, ref in enumerate((pair_o, pair_st)):
        remote(ref, ref, pair_send.at[which], pair_recv.at[0, which], mate).wait_send()
    for copy in a_copies:
        copy.wait_send()
    for which, count in enumerate((3, 4)):
        ref = w_v.at[c, pl.ds(0, count)]
        remote(ref, ref, w_send.at[which], w_recv.at[6], mate).wait_send()
    for first, count in ((True, 15), (False, 13)):

        @pl.when((z == 0) == first)
        def _():
            sent = x_all.at[pl.ds(0, count)]
            remote(sent, sent, d_send.at[1], d_recv.at[z], mate).wait_send()

    remote(others_e, others_e, e_send, e_recv, mate).wait_send()


def on_device(queries, keys, values, cached_length, out_weight):
    hbm = pl.BlockSpec(memory_space=pl.ANY)
    dma = pltpu.SemaphoreType.DMA
    out = pl.pallas_call(
        kernel,
        out_shape=pltpu.VMEM((16, 512), BF16),
        in_specs=[hbm] * 5,
        out_specs=pl.BlockSpec(memory_space=pltpu.VMEM),
        scratch_shapes=[
            pltpu.SMEM((4,), jnp.int32),
            pltpu.VMEM((2, 2, 4, 8192), BF16),
            pltpu.VMEM((2, 2, 8, 128, 128), BF16),
            pltpu.VMEM((2, 2, 8, 128, 128), BF16),
            pltpu.VMEM((2, 4, 512, 128), BF16),
            pltpu.VMEM((2, 4, 64, 128), BF16),
            pltpu.VMEM((2, 4, 128), F32),
            pltpu.VMEM((2, 4, 64, 128), BF16),
            pltpu.VMEM((2, 4, 128), F32),
            pltpu.VMEM((8, 64, 128), F32),
            pltpu.VMEM((2, 4, 128), F32),
            pltpu.VMEM((8, 64, 128), BF16),
            pltpu.VMEM((8, 1, 128), F32),
            pltpu.VMEM((8, 64, 128), BF16),
            pltpu.VMEM((8, 1, 128), F32),
            pltpu.VMEM((16, 8, 1024), BF16),
            pltpu.VMEM((16, 8, 512), BF16),
            pltpu.VMEM((16, 8, 512), BF16),
            pltpu.SemaphoreType.REGULAR,
            pltpu.SemaphoreType.REGULAR,
            dma,
            dma((2, 3)),
            dma,
            dma((2,)),
            dma((2, 2)),
            dma((2,)),
            dma((7,)),
            dma,
            dma,
            dma,
            dma,
            dma((2,)),
            dma((8,)),
            dma,
            dma,
        ],
        compiler_params=pltpu.CompilerParams(collective_id=0, has_side_effects=True),
        name="decode_step",
    )(cached_length, queries, keys, values, out_weight)
    return out.reshape(16, 4, 128)


def solution(mesh):
    in_specs = (
        P(("group", "dp"), None, None),
        P(("group", "dp"), None, "tensor", None),
        P(("group", "dp"), None, "tensor", None),
        P(("group", "dp")),
        P("tensor", ("group", "dp")),
    )
    out_specs = P(("group", "tensor"), None, "dp")
    return jax.shard_map(
        on_device, mesh=mesh, in_specs=in_specs, out_specs=out_specs, check_vma=False
    )
```

```python
import functools
import math

import jax
import jax.numpy as jnp
from jax import lax
from jax.experimental import pallas as pl
from jax.experimental.pallas import tpu as pltpu
from jax.sharding import PartitionSpec as P

MESH = pl.DeviceIdType.MESH
F32 = jnp.float32
BF16 = jnp.bfloat16
ORDER = (4, 3, 5, 2, 6, 1, 7, 0)


def remote(src, dst, send, recv, device):
    return pltpu.make_async_remote_copy(
        src_ref=src, dst_ref=dst, send_sem=send, recv_sem=recv, device_id=device, device_id_type=MESH
    )


def kernel(
    length_hbm,
    q_hbm,
    k_hbm,
    v_hbm,
    w_hbm,
    out_ref,
    length_ref,
    q_v,
    k_v,
    v_v,
    w_v,
    pair_o,
    pair_st,
    got_o,
    got_st,
    own_w,
    own_st,
    a_o,
    a_st,
    ar_o,
    ar_st,
    x_all,
    e_o,
    er_o,
    hello_sem,
    hello_x_sem,
    length_sem,
    load_sem,
    wload_sem,
    pair_send,
    pair_recv,
    w_send,
    w_recv,
    a_send,
    a_recv,
    ast_send,
    ast_recv,
    d_send,
    d_recv,
    e_send,
    e_recv,
):
    g = lax.axis_index("group")
    d = lax.axis_index("dp")
    t = lax.axis_index("tensor")
    x, c = t // 2, t % 2
    other = 1 - c
    ylo, z = d // 8, d % 8
    mate = {"tensor": x * 2 + other}
    right = {"group": (g + 1) % 4}
    left = {"group": (g + 3) % 4}

    def along_x(step, core):
        return {"tensor": ((x + step) % 8) * 2 + core}

    def plane(side, zz):
        return {"dp": (ylo if side == 0 else 1 - ylo) * 8 + zz}

    loads = []
    for slot, half in ((0, other), (1, c)):
        rows = pl.ds(half * 2, 2)
        for which, (src, dst) in enumerate(((q_hbm, q_v), (k_hbm, k_v), (v_hbm, v_v))):
            copy = pltpu.make_async_copy(src.at[rows], dst.at[slot], load_sem.at[slot, which])
            copy.start()
            loads.append(copy)
        if slot == 0:
            length_load = pltpu.make_async_copy(length_hbm, length_ref, length_sem)
            length_load.start()
    w_load = pltpu.make_async_copy(w_hbm, w_v.at[c, g], wload_sem)
    w_load.start()

    barrier = pltpu.get_barrier_semaphore()

    def greet(device):
        pl.semaphore_signal(barrier, inc=1, device_id=device, device_id_type=MESH)

    def rank_of(v):
        return v - 2 * (v // 5) * (v - 4)

    def along_x_if(test, act):
        for step in range(1, 8):

            @pl.when(test(rank_of((x + step) % 8), rank))
            def _():
                act(along_x(step, 0))
                act(along_x(step, 1))

    rank = rank_of(x)
    greet(mate)
    greet(plane(1, z))
    along_x_if(lambda theirs, mine: theirs >= mine, greet)
    pl.when((g == 0) | (g == 1))(lambda: greet(right))
    pl.when((g == 0) | (g == 3))(lambda: greet(left))
    for zz in range(1, 8):

        @pl.when(zz > z)
        def _():
            greet(plane(0, zz))
            greet(plane(1, zz))

    lane = lax.broadcasted_iota(jnp.int32, (64, 128), 1)
    row = lax.broadcasted_iota(jnp.int32, (64, 128), 0)
    first_row = (row // 4) % 2 == 0
    low_eye = lane == row
    high_eye = lane == row + 64
    position = t * 128 + lane
    scale = 1.0 / math.sqrt(128)

    def attend(slot, step, allowed):
        k = (x + step) % 8
        features = pl.ds(pl.multiple_of(k * 1024, 1024), 1024)
        pair = jnp.concatenate([q_v[slot, r, :, features].astype(F32) for r in range(2)], axis=0)
        q = jnp.concatenate([pair[:, j * 128 : (j + 1) * 128] for j in range(8)], axis=0).astype(BF16)
        keys = jnp.concatenate([k_v[slot, 0, k].T, k_v[slot, 1, k].T], axis=1)
        vals = jnp.concatenate([v_v[slot, 0, k], v_v[slot, 1, k]], axis=0)
        s = jnp.dot(q, keys, preferred_element_type=F32)
        s = jnp.where(first_row, s[:, :128], s[:, 128:]) * scale
        s = jnp.where(allowed, s, -1e30)
        m = jnp.max(s, axis=1, keepdims=True)
        p = jnp.where(allowed, jnp.exp(s - m), 0.0)
        l = jnp.sum(p, axis=1, keepdims=True)
        both = jnp.concatenate(
            [jnp.where(first_row, p, 0.0), jnp.where(first_row, 0.0, p)], axis=1
        ).astype(BF16)
        w = jnp.dot(both, vals, preferred_element_type=F32)
        stats = jnp.where(low_eye, m, jnp.where(high_eye, l, 0.0))
        return w, jnp.sum(stats, axis=0, keepdims=True)

    def mask_of(half):
        horizon = jnp.where(first_row, length_ref[half * 2], length_ref[half * 2 + 1]) + row % 4 + 1
        return position < horizon

    def attend_other(chunk):
        done = [attend(0, ORDER[chunk * 4 + i], allowed) for i in range(4)]
        for i, (w, stats) in enumerate(done):
            pair_o[chunk, i] = w.astype(BF16)
        pair_st[chunk] = jnp.concatenate([stats for _, stats in done], axis=0)

    pair_copies = []

    def send_pair(chunk):
        for which, (src, dst) in enumerate(((pair_o, got_o), (pair_st, got_st))):
            copy = remote(
                src.at[chunk], dst.at[chunk], pair_send.at[which], pair_recv.at[chunk, which], mate
            )
            copy.start()
            pair_copies.append(copy)

    before_x = 4 * rank - 2 * (rank // 4)
    pl.semaphore_wait(barrier, 2 + before_x + (g % 2) + 2 * ((g // 2) * (1 - g % 2)) + 2 * z)

    def hello(sem, device):
        pl.semaphore_signal(sem, inc=1, device_id=device, device_id_type=MESH)

    along_x_if(lambda theirs, mine: theirs < mine, lambda device: hello(hello_x_sem, device))
    pl.when((g == 1) | (g == 2))(lambda: hello(hello_sem, left))
    pl.when((g == 2) | (g == 3))(lambda: hello(hello_sem, right))

    length_load.wait()
    for copy in loads[:3]:
        copy.wait()
    allowed = mask_of(other)
    attend_other(0)
    send_pair(0)
    attend_other(1)
    send_pair(1)

    w_load.wait()
    top, bottom = pl.ds(0, 256), pl.ds(256, 256)

    def w_copy(block, part, index, device):
        ref = w_v.at[c, block, part]
        return remote(ref, ref, w_send.at[0], w_recv.at[index], device)

    w_top_right = w_copy(g, top, 0, right)
    w_bottom_left = w_copy(g, bottom, 1, left)
    w_bottom_right = w_copy(g, bottom, 2, right)
    w_top_left = w_copy(g, top, 3, left)

    def w_to_right():
        w_top_right.start()
        w_bottom_right.start()

    def w_to_left():
        w_bottom_left.start()
        w_top_left.start()

    def w_to_mate(block):
        ref = w_v.at[c, block]
        remote(ref, ref, w_send.at[1], w_recv.at[6], mate).start()

    pl.when((g == 1) | (g == 2))(w_to_left)
    pl.when((g == 2) | (g == 3))(w_to_right)

    for copy in loads[3:]:
        copy.wait()
    allowed = mask_of(c)
    for chunk in range(2):
        done = [attend(1, ORDER[chunk * 4 + i], allowed) for i in range(4)]
        for i, (w, stats) in enumerate(done):
            own_w[chunk * 4 + i] = w
        own_st[chunk] = jnp.concatenate([stats for _, stats in done], axis=0)

    a_copies = (
        remote(ar_o.at[pl.ds(1, 7)], ar_o.at[pl.ds(1, 7)], a_send, a_recv, mate),
        remote(ar_st.at[pl.ds(1, 7)], ar_st.at[pl.ds(1, 7)], ast_send, ast_recv, mate),
    )
    low = lax.broadcasted_iota(jnp.int32, (4, 128), 1) < 64
    for chunk in range(2):
        for copy in pair_copies[2 * chunk : 2 * chunk + 2]:
            copy.wait_recv()
        st1, st2 = own_st[chunk], got_st[chunk]
        top_both = jnp.maximum(st1, st2)
        e1, e2 = jnp.exp(st1 - top_both), jnp.exp(st2 - top_both)
        total = e1 * pltpu.roll(st1, 64, 1) + e2 * pltpu.roll(st2, 64, 1)
        merged = jnp.where(low, top_both, pltpu.roll(total, 64, 1))
        factors = jnp.where(low, e1, pltpu.roll(e2, 64, 1))
        for i in range(4):
            step = ORDER[chunk * 4 + i]
            f = factors[i : i + 1]
            f1 = jnp.sum(jnp.where(low_eye, f, 0.0), axis=1, keepdims=True)
            f2 = jnp.sum(jnp.where(high_eye, f, 0.0), axis=1, keepdims=True)
            a_o[step] = (f1 * own_w[chunk * 4 + i] + f2 * got_o[chunk, i].astype(F32)).astype(BF16)
            a_st[step] = merged[i : i + 1]
        if chunk == 0:
            pl.when(rank < 4)(lambda: pl.semaphore_wait(hello_x_sem, 14 - before_x))
        for i in range(4):
            step = ORDER[chunk * 4 + i]
            if step == 0:
                continue
            to = along_x(step, c)
            pair = (
                remote(a_o.at[step], ar_o.at[step], a_send, a_recv, to),
                remote(a_st.at[step], ar_st.at[step], ast_send, ast_recv, to),
            )
            for copy in pair:
                copy.start()

    pl.when(g != 2)(lambda: pl.semaphore_wait(hello_sem, 2 - g % 2))
    to_right, to_left = (g == 0) | (g == 1), (g == 0) | (g == 3)
    pl.when(to_right)(lambda: w_top_right.start())
    pl.when(to_left)(lambda: w_bottom_left.start())
    pl.when(to_right & (z < 4))(lambda: w_bottom_right.start())
    pl.when(to_left & (z < 4))(lambda: w_top_left.start())
    w_to_mate(g)
    w_on_right = w_copy((g + 3) % 4, top, 4, right)
    w_on_left = w_copy((g + 1) % 4, bottom, 5, left)

    def w_relay():
        w_top_right.wait_recv()
        w_on_right.start()
        w_bottom_left.wait_recv()
        w_on_left.start()

    pl.when(z < 4)(w_relay)

    for copy in a_copies:
        copy.wait_recv()
    st = jnp.concatenate([a_st[0]] + [ar_st[i] for i in range(1, 8)], axis=0)
    m = jnp.max(st, axis=0, keepdims=True)
    e = jnp.exp(st - m)
    total = jnp.sum(e * pltpu.roll(st, 64, 1), axis=0, keepdims=True)
    f = e / total
    attended = jnp.zeros((64, 128), F32)
    for i in range(8):
        part = a_o[0] if i == 0 else ar_o[i]
        fi = jnp.sum(jnp.where(low_eye, f[i : i + 1], 0.0), axis=1, keepdims=True)
        attended += fi * part.astype(F32)
    for j in range(8):
        x_all[d, :, j * 128 : (j + 1) * 128] = attended[j * 8 : (j + 1) * 8].astype(BF16)

    def d_copy(side, zz):
        ref = x_all.at[d]
        first = isinstance(zz, int) and zz == 0
        return remote(ref, ref, d_send.at[0 if first else 1], d_recv.at[z], plane(side, zz))

    def d_arrival(count, zz):
        ref = x_all.at[pl.ds(0, count)]
        return remote(ref, ref, d_send.at[1], d_recv.at[zz], plane(1, z))

    def d_start(zz):
        d_copy(1, zz).start()
        d_copy(0, zz).start()

    for zz in (0, 1, 3):
        pl.when(zz < z)(lambda: d_start(zz))

    @pl.when(z > 0)
    def _():
        two = x_all.at[pl.ds(0, 2)]
        remote(two, two, d_send.at[0], d_recv.at[z], mate).wait_send()

    pl.when(2 < z)(lambda: d_start(2))
    d_copy(1, z).start()
    pl.when(to_right & (z >= 4))(lambda: w_bottom_right.start())
    pl.when(to_left & (z >= 4))(lambda: w_top_left.start())
    pl.when(z >= 4)(w_relay)
    for zz in (4, 5, 6):
        pl.when(zz < z)(lambda: d_start(zz))
    w_bottom_right.wait_recv()
    w_to_mate((g + 3) % 4)
    w_top_left.wait_recv()
    w_to_mate((g + 1) % 4)

    def d_wait(zz):
        d_arrival(2, zz).wait_recv()

    for zz in range(1, 8):

        @pl.when((zz > z) & ((z >= 4) | (zz < 4)))
        def _():
            d_wait(zz)
            d_start(zz)

    w_on_right.wait_recv()
    w_on_left.wait_recv()
    w_to_mate((g + 2) % 4)
    remote(w_v.at[other], w_v.at[other], w_send.at[1], w_recv.at[6], mate).wait_recv()

    def e_copy(block):
        return remote(
            e_o.at[block], er_o.at[t], e_send, e_recv, {"tensor": jnp.asarray(block, jnp.int32)}
        )

    last = z // 7
    for i in range(8):
        if i == 0:
            zz = z
        elif i == 1:
            zz = (1 - last) * (z + 1)
        else:
            zz = last * (i - 1) + (1 - last) * (i - 2 * ((z + 9 - i) // 8))
        if i == 0:
            d_arrival(1, zz).wait_recv()
        else:
            pl.when((zz < z) | ((z < 4) & (zz >= 4)))(lambda: d_wait(zz))
            pl.when((z < 4) & (zz >= 4))(lambda: d_start(zz))
        blocks = (ylo * 8 + zz, (1 - ylo) * 8 + zz)
        tokens = jnp.concatenate([x_all[block].astype(F32) for block in blocks], axis=0).astype(BF16)
        for pair in range(2):
            y = jnp.zeros((16, 256), F32)
            for side in range(2):
                weight = jnp.concatenate([w_v[side, 2 * pair], w_v[side, 2 * pair + 1]], axis=1)
                y += jnp.dot(tokens[:, side * 512 : (side + 1) * 512], weight, preferred_element_type=F32)
            for side in range(2):
                e_o[blocks[side], :, pair * 256 : (pair + 1) * 256] = y[side * 8 : (side + 1) * 8].astype(BF16)
        for block in blocks:
            pl.when(block != t)(lambda: e_copy(block).start())

    er_o[t] = e_o[t]
    others_e = er_o.at[pl.ds(0, 15)]
    remote(others_e, others_e, e_send, e_recv, mate).wait_recv()

    result = []
    for core in range(2):
        summed = er_o[core].astype(F32)
        for step in range(1, 8):
            summed += er_o[2 * step + core].astype(F32)
        result.append(summed)
    out_ref[...] = jnp.concatenate(result, axis=0).astype(BF16)

    for which, ref in enumerate((pair_o, pair_st)):
        remote(ref, ref, pair_send.at[which], pair_recv.at[0, which], mate).wait_send()
    for copy in a_copies:
        copy.wait_send()
    for which, count in enumerate((3, 4)):
        ref = w_v.at[c, pl.ds(0, count)]
        remote(ref, ref, w_send.at[which], w_recv.at[6], mate).wait_send()
    for first, count in ((True, 15), (False, 13)):

        @pl.when((z == 0) == first)
        def _():
            sent = x_all.at[pl.ds(0, count)]
            remote(sent, sent, d_send.at[1], d_recv.at[z], mate).wait_send()

    remote(others_e, others_e, e_send, e_recv, mate).wait_send()


def on_device(queries, keys, values, cached_length, out_weight):
    hbm = pl.BlockSpec(memory_space=pl.ANY)
    dma = pltpu.SemaphoreType.DMA
    out = pl.pallas_call(
        kernel,
        out_shape=pltpu.VMEM((16, 512), BF16),
        in_specs=[hbm] * 5,
        out_specs=pl.BlockSpec(memory_space=pltpu.VMEM),
        scratch_shapes=[
            pltpu.SMEM((4,), jnp.int32),
            pltpu.VMEM((2, 2, 4, 8192), BF16),
            pltpu.VMEM((2, 2, 8, 128, 128), BF16),
            pltpu.VMEM((2, 2, 8, 128, 128), BF16),
            pltpu.VMEM((2, 4, 512, 128), BF16),
            pltpu.VMEM((2, 4, 64, 128), BF16),
            pltpu.VMEM((2, 4, 128), F32),
            pltpu.VMEM((2, 4, 64, 128), BF16),
            pltpu.VMEM((2, 4, 128), F32),
            pltpu.VMEM((8, 64, 128), F32),
            pltpu.VMEM((2, 4, 128), F32),
            pltpu.VMEM((8, 64, 128), BF16),
            pltpu.VMEM((8, 1, 128), F32),
            pltpu.VMEM((8, 64, 128), BF16),
            pltpu.VMEM((8, 1, 128), F32),
            pltpu.VMEM((16, 8, 1024), BF16),
            pltpu.VMEM((16, 8, 512), BF16),
            pltpu.VMEM((16, 8, 512), BF16),
            pltpu.SemaphoreType.REGULAR,
            pltpu.SemaphoreType.REGULAR,
            dma,
            dma((2, 3)),
            dma,
            dma((2,)),
            dma((2, 2)),
            dma((2,)),
            dma((7,)),
            dma,
            dma,
            dma,
            dma,
            dma((2,)),
            dma((8,)),
            dma,
            dma,
        ],
        compiler_params=pltpu.CompilerParams(collective_id=0, has_side_effects=True),
        name="decode_step",
    )(cached_length, queries, keys, values, out_weight)
    return out.reshape(16, 4, 128)


def solution(mesh):
    in_specs = (
        P(("group", "dp"), None, None),
        P(("group", "dp"), None, "tensor", None),
        P(("group", "dp"), None, "tensor", None),
        P(("group", "dp")),
        P("tensor", ("group", "dp")),
    )
    out_specs = P(("group", "tensor"), None, "dp")
    return jax.shard_map(
        on_device, mesh=mesh, in_specs=in_specs, out_specs=out_specs, check_vma=False
    )
```
